16 devices in a mesh: rep: 4 (over y, z, core), dp: 4 (over x).
Axes of the slice: x: 4, y: 2, z: 1, core: 2. Of those that a mesh axis runs over, the one named last changes fastest.
The devices are a block of a 4x4x8 slice.
Arguments:
- x: bfloat16 [16, 2048, 1024], P(('rep', 'dp')), parts along dimension 0
- dy: bfloat16 [16, 2048, 1024], P(('rep', 'dp')), parts along dimension 0
- wq: bfloat16 [2, 1024, 1024], P(None, 'dp')
- wk: bfloat16 [2, 1024, 256], P(None, 'dp')
- wv: bfloat16 [2, 1024, 256], P(None, 'dp')
- wo: bfloat16 [2, 1024, 1024], P(None, 'dp')
- w_gate: bfloat16 [2, 1024, 3200], P(None, 'dp')
- w_up: bfloat16 [2, 1024, 3200], P(None, 'dp')
- w_down: bfloat16 [2, 3200, 1024], P(None, 'dp')
Outputs:
- output 1: bfloat16 [16, 2048, 1024], P(('rep', 'dp')), parts along dimension 0
- output 2: bfloat16 [8, 1024, 1024], P('rep', 'dp'), parts along dimension 0
- output 3: bfloat16 [8, 1024, 256], P('rep', 'dp'), parts along dimension 0
- output 4: bfloat16 [8, 1024, 256], P('rep', 'dp'), parts along dimension 0
- output 5: bfloat16 [8, 1024, 1024], P('rep', 'dp'), parts along dimension 0
- output 6: bfloat16 [8, 1024, 3200], P('rep', 'dp'), parts along dimension 0
- output 7: bfloat16 [8, 1024, 3200], P('rep', 'dp'), parts along dimension 0
- output 8: bfloat16 [8, 3200, 1024], P('rep', 'dp'), parts along dimension 0
There are 4 independent parts. The reference program is written for one: setup_inputs(seed, part) draws one part's arguments, and reference() takes and returns one part's arrays. A program takes and returns all parts, laid end to end along the dimension named above; an argument that names none is the same for every part.
All inputs are finite; a program needn't handle non-finite values.
Results may differ from the reference program's by a relative error of at most 0.0288.
Values are sent between devices in bfloat16 or wider.
A program may use at most 768 MiB of HBM per device.

```python
import jax
import jax.numpy as jnp
from jax import lax

SEQUENCES = 4
TOKENS = 2048
D = 1024
HEADS = 8
KV_HEADS = 2
HEAD = 128
FF = 3200
LAYERS = 2
THETA = 10000
NAMES = ("wq", "wk", "wv", "wo", "w_gate", "w_up", "w_down")
SHAPES = {
    "wq": (LAYERS, D, HEADS * HEAD),
    "wk": (LAYERS, D, KV_HEADS * HEAD),
    "wv": (LAYERS, D, KV_HEADS * HEAD),
    "wo": (LAYERS, HEADS * HEAD, D),
    "w_gate": (LAYERS, D, FF),
    "w_up": (LAYERS, D, FF),
    "w_down": (LAYERS, FF, D),
}


def bump(key, n, height):
    away = (jnp.arange(n, dtype=jnp.int32) - jax.random.randint(key, (), 0, n, jnp.int32)) % n
    return jnp.where(away < n // 8, height, 1.0)


def together(key, own, strength):
    shared = jax.random.normal(key, own.shape[1:], jnp.float32)
    return (own + strength * shared) * lax.rsqrt(1 + strength * strength)


def setup_inputs(seed: int = 0, part: int = 0) -> dict:
    kx, kdy, ka, kb, kz, kf, kh, kl, *keys = jax.random.split(jax.random.key(seed), 8 + 3 * len(NAMES))
    kx, kdy, ka, kb = (jax.random.fold_in(k, part) for k in (kx, kdy, ka, kb))
    kw, km, kv = (keys[i::3] for i in range(3))
    shape = (SEQUENCES, TOKENS, D)
    much_x, much_dy = jax.random.uniform(kz, (2,), jnp.float32, 0.0, 1.0)
    loud = 2.0 ** jax.random.uniform(jax.random.fold_in(kz, 1), (), jnp.float32, -1.0, 2.0)
    layers = 2.0 ** jax.random.uniform(kl, (LAYERS, 1, 1), jnp.float32, -1.0, 1.0)
    times = {"wq": 1.0, "wk": 1.0, "wv": 2.0, "wo": layers, "w_gate": 1.0, "w_up": bump(kh, FF, 4.0), "w_down": layers}
    x = together(ka, jax.random.normal(kx, shape, jnp.float32), much_x) * bump(kf, D, 4.0)
    dy = together(kb, jax.random.normal(kdy, shape, jnp.float32), much_dy)
    drawn = {"x": x.astype(jnp.bfloat16), "dy": (loud * dy * (SEQUENCES * TOKENS) ** -0.5).astype(jnp.bfloat16)}
    for key, name in zip(kw, NAMES, strict=True):
        drawn[name] = (jax.random.normal(key, SHAPES[name], jnp.float32) * SHAPES[name][1] ** -0.5 * times[name]).astype(jnp.bfloat16)
    return drawn


def matmul(a, w):
    return jnp.dot(a, w, preferred_element_type=jnp.float32).astype(jnp.bfloat16)


def normed(h):
    wide = h.astype(jnp.float32)
    scale = lax.rsqrt(jnp.mean(wide**2, -1, keepdims=True) + 1e-6)
    return (wide * scale).astype(jnp.bfloat16)


def turned(t, theta):
    half = t.shape[-1] // 2
    angle = jnp.arange(t.shape[0], dtype=jnp.float32)[:, None] * theta ** (-jnp.arange(half, dtype=jnp.float32) / half)
    cos, sin = jnp.cos(angle)[:, None], jnp.sin(angle)[:, None]
    a, b = t[..., :half].astype(jnp.float32), t[..., half:].astype(jnp.float32)
    return jnp.concatenate([a * cos - b * sin, b * cos + a * sin], -1).astype(jnp.bfloat16)


def seen_by(q, k, v):
    tokens, kv = q.shape[0], k.shape[1]
    q = q.reshape(tokens, kv, -1, q.shape[-1])
    scores = jnp.einsum("tgsd,ugd->gstu", q.astype(jnp.float32), k.astype(jnp.float32)) * q.shape[-1] ** -0.5
    place = jnp.arange(tokens)
    weights = jax.nn.softmax(jnp.where(place[:, None] >= place, scores, -jnp.inf), -1).astype(jnp.bfloat16)
    return jnp.einsum("gstu,ugd->tgsd", weights.astype(jnp.float32), v.astype(jnp.float32)).astype(jnp.bfloat16).reshape(tokens, -1)


def layer(h, w):
    a = normed(h)
    q, k = (turned(matmul(a, w[name]).reshape(h.shape[0], -1, HEAD), THETA) for name in ("wq", "wk"))
    h = h + matmul(seen_by(q, k, matmul(a, w["wv"]).reshape(h.shape[0], -1, HEAD)), w["wo"])
    b = normed(h)
    gate = jnp.dot(b, w["w_gate"], preferred_element_type=jnp.float32)
    up = jnp.dot(b, w["w_up"], preferred_element_type=jnp.float32)
    return h + matmul((jax.nn.silu(gate) * up).astype(jnp.bfloat16), w["w_down"])


def stack(weights, h):
    return lax.scan(lambda h, w: (layer(h, w), None), h, weights)[0]


def reference(x, dy, wq, wk, wv, wo, w_gate, w_up, w_down):
    weights = dict(zip(NAMES, (wq, wk, wv, wo, w_gate, w_up, w_down), strict=True))

    def take(so_far, sequence):
        h, by_y = sequence
        _, back = jax.vjp(stack, weights, h)
        by_weights, by_h = back(by_y)
        return jax.tree.map(lambda total, term: total + term.astype(jnp.float32), so_far, by_weights), by_h

    none_yet = {name: jnp.zeros(w.shape, jnp.float32) for name, w in weights.items()}
    by_weights, by_x = lax.scan(take, none_yet, (x, dy))
    return (by_x, *(by_weights[name].astype(jnp.bfloat16) for name in NAMES))
```

```python
import functools

import jax
import jax.numpy as jnp
from jax import lax
from jax.experimental import pallas as pl
from jax.experimental.pallas import tpu as pltpu
from jax.sharding import PartitionSpec as P

NAMES = ("wq", "wk", "wv", "wo", "w_gate", "w_up", "w_down")
THETA = 10000
NEG=-1e30
LOG2E=1.4426950408889634
HEAD=128
bf16=jnp.bfloat16; f32=jnp.float32

def _dot(a, b, ca, cb):
    return lax.dot_general(a, b, (((ca,), (cb,)), ((), ())), preferred_element_type=jnp.float32)

def _fwd(q_ref,k_ref,v_ref,o_ref,lse_ref,top_s,mix_s,*,bq,bk,sub):
    iq=pl.program_id(0)
    heads=q_ref.shape[1]//HEAD; kv=k_ref.shape[1]//HEAD; g=heads//kv
    scale=HEAD**-0.5; e=scale*LOG2E
    top_s[...]=jnp.full(top_s.shape,NEG,f32)
    mix_s[...]=jnp.zeros(mix_s.shape,f32)
    def head(n): return slice(n*HEAD,(n+1)*HEAD)
    def block(rows,size,lo,masked):
        ones=jnp.ones((8,size),bf16)
        scores=[_dot(k_ref[rows,head(n//g)],q_ref[lo:,head(n)],1,1) for n in range(heads)]
        weights,keeps=[],[]
        if masked:
            ok=lax.broadcasted_iota(jnp.int32,(size,bq-lo),1)>=lax.broadcasted_iota(jnp.int32,(size,bq-lo),0)
        for n in range(heads):
            s=scores[n]
            if masked: s=jnp.where(ok,s,2*NEG)
            old=top_s[n:n+1,lo:]
            top=jnp.maximum(old,s.max(axis=0,keepdims=True))
            top_s[n:n+1,lo:]=top
            weights.append(jnp.exp2((s-top)*e).astype(bf16))
            keeps.append(jnp.exp2((old-top)*e))
        for n in range(heads):
            values=jnp.concatenate([v_ref[rows,head(n//g)].T,ones],axis=0)
            mix_s[n,:,lo:]=mix_s[n,:,lo:]*keeps[n]+_dot(values,weights[n],1,0)
    lax.fori_loop(0,iq*(bq//bk),lambda j,_: block(pl.ds(pl.multiple_of(j*bk,bk),bk),bk,0,False),None)
    for at in range(0,bq,sub):
        block(pl.ds(pl.multiple_of(iq*bq+at,sub),sub),sub,at,True)
    for n in range(heads):
        top,total=top_s[n:n+1,:],mix_s[n,HEAD:HEAD+1,:]
        o_ref[:,head(n)]=(mix_s[n,:HEAD,:]*(1/total)).T.astype(bf16)
        lse_ref[n:n+1,:]=top*scale+jnp.log(total)

def attend(q,k,v,bq=512,bk=512,sub=256):
    t=q.shape[0]; heads=q.shape[1]//HEAD
    rows=lambda w: pl.BlockSpec((bq,w),lambda i:(i,0))
    whole=lambda a: pl.BlockSpec(a.shape,lambda i:(0,0))
    return pl.pallas_call(functools.partial(_fwd,bq=bq,bk=bk,sub=sub),grid=(t//bq,),
        in_specs=[rows(q.shape[1]),whole(k),whole(v)],
        out_specs=[rows(q.shape[1]),pl.BlockSpec((heads,bq),lambda i:(0,i))],
        out_shape=[jax.ShapeDtypeStruct(q.shape,bf16),jax.ShapeDtypeStruct((heads,t),f32)],
        scratch_shapes=[pltpu.VMEM((heads,bq),f32),pltpu.VMEM((heads,HEAD+8,bq),f32)],
        compiler_params=pltpu.CompilerParams(dimension_semantics=("arbitrary",),vmem_limit_bytes=60*2**20),name="attend",
        cost_estimate=pl.CostEstimate(flops=4*t*t//2*q.shape[1],transcendentals=heads*t*t//2,bytes_accessed=4*q.size*2))(q,k,v)

def _bwd(q_ref,k_ref,v_ref,do_ref,o_ref,lse_ref,dq_ref,dk_ref,dv_ref,q_s,do_s,dq_s,dk_s,dv_s,row_s,*,bq,bk):
    iq=pl.program_id(0)
    heads=q_ref.shape[1]//HEAD; kv=k_ref.shape[1]//HEAD; g=heads//kv; cols=g*bq
    scale=HEAD**-0.5; e=scale*LOG2E
    def head(n): return slice(n*HEAD,(n+1)*HEAD)
    @pl.when(iq==0)
    def _():
        dk_s[...]=jnp.zeros_like(dk_s); dv_s[...]=jnp.zeros_like(dv_s)
    for n in range(heads):
        i,at=n//g,(n%g)*bq
        q_s[i,at:at+bq,:]=q_ref[:,head(n)]
        do_s[i,at:at+bq,:]=do_ref[:,head(n)]
        row_s[i,0:1,at:at+bq]=lse_ref[n:n+1,:]*LOG2E
        row_s[i,1:2,at:at+bq]=jnp.sum((do_ref[:,head(n)].astype(f32)*o_ref[:,head(n)].astype(f32)).T,axis=0,keepdims=True)
    dq_s[...]=jnp.zeros_like(dq_s)
    def block(rows,size,masked):
        if masked:
            ok=lax.rem(lax.broadcasted_iota(jnp.int32,(size,cols),1),bq)>=lax.broadcasted_iota(jnp.int32,(size,cols),0)
        for i in range(kv):
            s=_dot(k_ref[rows,head(i)],q_s[i],1,1)
            dp=_dot(v_ref[rows,head(i)],do_s[i],1,1)
            p=jnp.exp2(s*e-row_s[i,0:1,:])
            if masked: p=jnp.where(ok,p,0.0)
            ds=(p*(dp-row_s[i,1:2,:])).astype(bf16)
            dv_s[i,rows,:]+=_dot(p.astype(bf16),do_s[i],1,0)
            dk_s[i,rows,:]+=_dot(ds,q_s[i],1,0)
            dq_s[i]+=_dot(k_ref[rows,head(i)].T,ds,1,0)
    lax.fori_loop(0,iq*(bq//bk),lambda j,_: block(pl.ds(pl.multiple_of(j*bk,bk),bk),bk,False),None)
    block(pl.ds(pl.multiple_of(iq*bq,bq),bq),bq,True)
    for n in range(heads):
        i,at=n//g,(n%g)*bq
        dq_ref[:,head(n)]=(dq_s[i,:,at:at+bq]*scale).T.astype(bf16)
    @pl.when(iq==pl.num_programs(0)-1)
    def _():
        for i in range(kv):
            dk_ref[:,head(i)]=(dk_s[i]*scale).astype(bf16)
            dv_ref[:,head(i)]=dv_s[i].astype(bf16)

def attend_bwd(q,k,v,do,o,lse,bq=256,bk=256):
    t=q.shape[0]; heads=q.shape[1]//HEAD; kv=k.shape[1]//HEAD; cols=heads//kv*bq
    rows=lambda w: pl.BlockSpec((bq,w),lambda i:(i,0))
    whole=lambda a: pl.BlockSpec(a.shape,lambda i:(0,0))
    return pl.pallas_call(functools.partial(_bwd,bq=bq,bk=bk),grid=(t//bq,),
        in_specs=[rows(q.shape[1]),whole(k),whole(v),rows(q.shape[1]),rows(q.shape[1]),pl.BlockSpec((heads,bq),lambda i:(0,i))],
        out_specs=[rows(q.shape[1]),whole(k),whole(v)],
        out_shape=[jax.ShapeDtypeStruct(a.shape,bf16) for a in (q,k,v)],
        scratch_shapes=[pltpu.VMEM((kv,cols,HEAD),bf16),pltpu.VMEM((kv,cols,HEAD),bf16),pltpu.VMEM((kv,HEAD,cols),f32),
            pltpu.VMEM((kv,t,HEAD),f32),pltpu.VMEM((kv,t,HEAD),f32),pltpu.VMEM((kv,8,cols),f32)],
        compiler_params=pltpu.CompilerParams(dimension_semantics=("arbitrary",),vmem_limit_bytes=60*2**20),name="attend_bwd",
        cost_estimate=pl.CostEstimate(flops=10*t*t//2*q.shape[1],transcendentals=heads*t*t//2,bytes_accessed=6*q.size*2))(q,k,v,do,o,lse)
VMEM=62*2**20
def _params(): return pltpu.CompilerParams(dimension_semantics=("arbitrary",),vmem_limit_bytes=VMEM)
def _cost(flops,nbytes,trans=0): return pl.CostEstimate(flops=int(flops),transcendentals=int(trans),bytes_accessed=int(nbytes))
ANY=pl.BlockSpec(memory_space=pl.ANY)
def rows(n,w): return pl.BlockSpec((n,w),lambda i:(i,0))
def whole(shape): return pl.BlockSpec(shape,lambda i:(0,)*len(shape))

class Weight:
    def __init__(self,shape,pieces,plan): self.shape,self.pieces,self.plan=shape,pieces,plan
    @property
    def n(self): return len(self.pieces)
    def copies(self,refs,dst,sem,col=0):
        x,c=lax.axis_index("dp"),lax.rem(lax.axis_index("rep"),2)
        out=[]
        for piece,src,size,at in self.plan:
            to=dst.at[pl.ds(pl.multiple_of(at(x,c),16),size),pl.ds(col,self.shape[1])]
            out.append(pltpu.make_async_copy(refs[piece].at[pl.ds(src,size)],to,sem))
        return out

def fetch(copies):
    for c in copies: c.start()
def arrive(copies):
    for c in copies: c.wait()

def split(refs,*counts):
    out=[];at=0
    for n in counts: out.append(refs[at:at+n]); at+=n
    return out

def rms_scale(wide): return lax.rsqrt(jnp.mean(wide*wide,-1,keepdims=True)+1e-6)

def normed(h):
    wide=h.astype(f32)
    return (wide*rms_scale(wide)).astype(bf16)

def turn(t,cos,sin):
    return t*cos+pltpu.roll(t,HEAD//2,1)*sin

def norm_qkv(h,cos,sin,w_s,a_ref,q_ref,k_ref,v_ref):
    a=normed(h)
    a_ref[...]=a
    nq,nk=q_ref.shape[1],k_ref.shape[1]
    y=_dot(a,w_s[...],1,0)
    for n in range(nq//HEAD):
        q_ref[:,n*HEAD:(n+1)*HEAD]=turn(y[:,n*HEAD:(n+1)*HEAD].astype(bf16).astype(f32),cos,sin).astype(bf16)
    for n in range(nk//HEAD):
        k_ref[:,n*HEAD:(n+1)*HEAD]=turn(y[:,nq+n*HEAD:nq+(n+1)*HEAD].astype(bf16).astype(f32),cos,sin).astype(bf16)
    v_ref[...]=y[:,nq+nk:].astype(bf16)

def qkv(h,cos,sin,wq,wk,wv,bm=512):
    t,d=h.shape; nq,nk=wq.shape[1],wk.shape[1]; n=nq+2*nk
    def body(h_ref,cos_ref,sin_ref,*rest):
        wqr,wkr,wvr,(a_ref,q_ref,k_ref,v_ref,w_s,sem)=split(rest,wq.n,wk.n,wv.n,6)
        @pl.when(pl.program_id(0)==0)
        def _():
            c=wq.copies(wqr,w_s,sem.at[0])+wk.copies(wkr,w_s,sem.at[0],nq)+wv.copies(wvr,w_s,sem.at[0],nq+nk)
            fetch(c); arrive(c)
        norm_qkv(h_ref[...],cos_ref[...],sin_ref[...],w_s,a_ref,q_ref,k_ref,v_ref)
    return pl.pallas_call(body,grid=(t//bm,),
        in_specs=[rows(bm,d),rows(bm,HEAD),rows(bm,HEAD)]+[ANY]*(wq.n+wk.n+wv.n),
        out_specs=[rows(bm,d),rows(bm,nq),rows(bm,nk),rows(bm,nk)],
        out_shape=[jax.ShapeDtypeStruct((t,w),bf16) for w in (d,nq,nk,nk)],
        scratch_shapes=[pltpu.VMEM((d,n),bf16),pltpu.SemaphoreType.DMA((1,))],
        compiler_params=_params(),name="qkv",cost_estimate=_cost(2*t*d*n,2*(t*2*d+t*n+d*n)))(h,cos,sin,*wq.pieces,*wk.pieces,*wv.pieces)

def out_norm(o,h,wo,bm=512):
    t,n=o.shape; d=h.shape[1]
    def body(o_ref,h_ref,*rest):
        wr,(h1_ref,b_ref,w_s,sem)=split(rest,wo.n,4)
        @pl.when(pl.program_id(0)==0)
        def _():
            c=wo.copies(wr,w_s,sem.at[0]); fetch(c); arrive(c)
        h1=h_ref[...]+_dot(o_ref[...],w_s[...],1,0).astype(bf16)
        h1_ref[...]=h1
        b_ref[...]=normed(h1)
    return pl.pallas_call(body,grid=(t//bm,),in_specs=[rows(bm,n),rows(bm,d)]+[ANY]*wo.n,out_specs=[rows(bm,d)]*2,
        out_shape=[jax.ShapeDtypeStruct((t,d),bf16)]*2,scratch_shapes=[pltpu.VMEM((n,d),bf16),pltpu.SemaphoreType.DMA((1,))],
        compiler_params=_params(),name="out_norm",cost_estimate=_cost(2*t*d*n,2*(4*t*d+d*n)))(o,h,*wo.pieces)

def chunks(f,size=1024):
    n=max(f//size,1)
    return [(i*size,(i+1)*size if i<n-1 else f) for i in range(n)]

def mlp_in(b,wg,wu,bm=512):
    t,d=b.shape; f=wg.shape[1]
    def body(b_ref,*rest):
        gr,ur,(gate_ref,up_ref,act_ref,wg_s,wu_s,sem)=split(rest,wg.n,wu.n,6)
        @pl.when(pl.program_id(0)==0)
        def _():
            c=wg.copies(gr,wg_s,sem.at[0])+wu.copies(ur,wu_s,sem.at[1]); fetch(c); arrive(c)
        for lo,hi in chunks(f):
            gate=_dot(b_ref[...],wg_s[:,lo:hi],1,0)
            up=_dot(b_ref[...],wu_s[:,lo:hi],1,0)
            gate_ref[:,lo:hi]=gate
            up_ref[:,lo:hi]=up
            act_ref[:,lo:hi]=(gate*jax.nn.sigmoid(gate)*up).astype(bf16)
    return pl.pallas_call(body,grid=(t//bm,),in_specs=[rows(bm,d)]+[ANY]*(wg.n+wu.n),out_specs=[rows(bm,f)]*3,
        out_shape=[jax.ShapeDtypeStruct((t,f),f32)]*2+[jax.ShapeDtypeStruct((t,f),bf16)],
        scratch_shapes=[pltpu.VMEM((d,f),bf16)]*2+[pltpu.SemaphoreType.DMA((2,))],
        compiler_params=_params(),name="mlp_in",cost_estimate=_cost(4*t*d*f,2*t*d+10*t*f+4*d*f,2*t*f))(b,*wg.pieces,*wu.pieces)

def mlp_out_qkv(act,h,wd,cos,sin,wq,wk,wv,bm=512):
    t,f=act.shape; d=h.shape[1]; nq,nk=wq.shape[1],wk.shape[1]; n=nq+2*nk
    def body(act_ref,h_ref,cos_ref,sin_ref,*rest):
        dr,wqr,wkr,wvr,(h_out,a_ref,q_ref,k_ref,v_ref,wd_s,w_s,sem)=split(rest,wd.n,wq.n,wk.n,wv.n,8)
        @pl.when(pl.program_id(0)==0)
        def _():
            c=wd.copies(dr,wd_s,sem.at[0])
            c+=wq.copies(wqr,w_s,sem.at[1])+wk.copies(wkr,w_s,sem.at[1],nq)+wv.copies(wvr,w_s,sem.at[1],nq+nk)
            fetch(c); arrive(c)
        h2=h_ref[...]+_dot(act_ref[...],wd_s[...],1,0).astype(bf16)
        h_out[...]=h2
        norm_qkv(h2,cos_ref[...],sin_ref[...],w_s,a_ref,q_ref,k_ref,v_ref)
    return pl.pallas_call(body,grid=(t//bm,),
        in_specs=[rows(bm,f),rows(bm,d),rows(bm,HEAD),rows(bm,HEAD)]+[ANY]*(wd.n+wq.n+wk.n+wv.n),
        out_specs=[rows(bm,d),rows(bm,d),rows(bm,nq),rows(bm,nk),rows(bm,nk)],
        out_shape=[jax.ShapeDtypeStruct((t,w),bf16) for w in (d,d,nq,nk,nk)],
        scratch_shapes=[pltpu.VMEM((f,d),bf16),pltpu.VMEM((d,n),bf16),pltpu.SemaphoreType.DMA((2,))],
        compiler_params=_params(),name="mlp_out_qkv",
        cost_estimate=_cost(2*t*d*(n+f),2*(t*f+t*3*d+t*n+d*n+d*f)))(act,h,cos,sin,*wd.pieces,*wq.pieces,*wk.pieces,*wv.pieces)

def outer(a,g,block):
    t,m=a.shape; n=g.shape[1]
    def body(a_ref,g_ref,o_ref): o_ref[...]=_dot(a_ref[...],g_ref[...],0,0).astype(bf16)
    return pl.pallas_call(body,grid=(m//block,),in_specs=[pl.BlockSpec((t,block),lambda i:(0,i)),whole(g.shape)],
        out_specs=rows(block,n),out_shape=jax.ShapeDtypeStruct((m,n),bf16),compiler_params=_params(),name="outer",
        cost_estimate=_cost(2*t*m*n,2*(t*m+t*n+m*n)))(a,g)

def outer_k(a,g,bm=512):
    t,m=a.shape; n=g.shape[1]; steps=t//bm
    def body(a_ref,g_ref,o_ref,acc):
        i=pl.program_id(0)
        y=lambda: _dot(a_ref[...],g_ref[...],0,0)
        @pl.when(i==0)
        def _(): acc[...]=y()
        @pl.when((i>0)&(i<steps-1))
        def _(): acc[...]+=y()
        @pl.when(i==steps-1)
        def _(): o_ref[...]=(acc[...]+y()).astype(bf16)
    return pl.pallas_call(body,grid=(steps,),in_specs=[rows(bm,m),rows(bm,n)],out_specs=whole((m,n)),
        out_shape=jax.ShapeDtypeStruct((m,n),bf16),scratch_shapes=[pltpu.VMEM((m,n),f32)],compiler_params=_params(),name="outer_k",
        cost_estimate=_cost(2*t*m*n,2*(t*m+t*n+m*n)))(a,g)

def norm_back(by_a,wide):
    scale=rms_scale(wide)
    return by_a*scale-wide*(scale*scale*scale*jnp.mean(by_a*wide,-1,keepdims=True))

def mlp_back(by_h,gate,up,h,wg,wu,wd,bm=256):
    t,d=by_h.shape; f=gate.shape[1]
    def body(by_ref,gate_ref,up_ref,h_ref,*rest):
        gr,ur,dr,(bg_ref,bu_ref,out_ref,wg_s,wu_s,wd_s,sem)=split(rest,wg.n,wu.n,wd.n,7)
        @pl.when(pl.program_id(0)==0)
        def _():
            c=wd.copies(dr,wd_s,sem.at[0])+wg.copies(gr,wg_s,sem.at[1])+wu.copies(ur,wu_s,sem.at[2]); fetch(c); arrive(c)
        for lo,hi in chunks(f):
            by_act=_dot(by_ref[...],wd_s[lo:hi,:],1,1).astype(bf16).astype(f32)
            gate=gate_ref[:,lo:hi]
            s=jax.nn.sigmoid(gate)
            bu_ref[:,lo:hi]=(by_act*(gate*s)).astype(bf16)
            bg_ref[:,lo:hi]=(by_act*up_ref[:,lo:hi]*(s+gate*s*(1-s))).astype(bf16)
        by_b=(_dot(bg_ref[...],wg_s[...],1,1)+_dot(bu_ref[...],wu_s[...],1,1)).astype(bf16).astype(f32)
        out_ref[...]=by_ref[...]+norm_back(by_b,h_ref[...].astype(f32)).astype(bf16)
    return pl.pallas_call(body,grid=(t//bm,),in_specs=[rows(bm,d),rows(bm,f),rows(bm,f),rows(bm,d)]+[ANY]*(wg.n+wu.n+wd.n),
        out_specs=[rows(bm,f),rows(bm,f),rows(bm,d)],out_shape=[jax.ShapeDtypeStruct((t,w),bf16) for w in (f,f,d)],
        scratch_shapes=[pltpu.VMEM((d,f),bf16)]*2+[pltpu.VMEM((f,d),bf16),pltpu.SemaphoreType.DMA((3,))],
        compiler_params=_params(),name="mlp_back",
        cost_estimate=_cost(6*t*d*f,6*t*d+12*t*f+6*d*f,2*t*f))(by_h,gate,up,h,*wg.pieces,*wu.pieces,*wd.pieces)

def out_back(by_h,o,wo,bm=512):
    t,d=by_h.shape; n=o.shape[1]; steps=t//bm
    def body(by_ref,o_ref,*rest):
        wr,(do_ref,dw_ref,w_s,acc,sem)=split(rest,wo.n,5)
        i=pl.program_id(0)
        @pl.when(i==0)
        def _():
            c=wo.copies(wr,w_s,sem.at[0]); fetch(c); acc[...]=jnp.zeros_like(acc); arrive(c)
        acc[...]+=_dot(o_ref[...],by_ref[...],0,0)
        do_ref[...]=_dot(by_ref[...],w_s[...],1,1).astype(bf16)
        @pl.when(i==steps-1)
        def _(): dw_ref[...]=acc[...].astype(bf16)
    return pl.pallas_call(body,grid=(steps,),in_specs=[rows(bm,d),rows(bm,n)]+[ANY]*wo.n,out_specs=[rows(bm,n),whole((n,d))],
        out_shape=[jax.ShapeDtypeStruct((t,n),bf16),jax.ShapeDtypeStruct((n,d),bf16)],
        scratch_shapes=[pltpu.VMEM((n,d),bf16),pltpu.VMEM((n,d),f32),pltpu.SemaphoreType.DMA((1,))],
        compiler_params=_params(),name="out_back",cost_estimate=_cost(4*t*d*n,2*(3*t*d+2*d*n)))(by_h,o,*wo.pieces)

def qkv_back(dq,dk,dv,a,h,by_h,cos,sin,wq,wk,wv,bm=512):
    t,d=h.shape; nq,nk=wq.shape[1],wk.shape[1]; n=nq+2*nk; steps=t//bm
    def body(dq_ref,dk_ref,dv_ref,a_ref,h_ref,by_ref,cos_ref,sin_ref,*rest):
        wqr,wkr,wvr,(out_ref,dw_ref,w_s,g_s,acc,sem)=split(rest,wq.n,wk.n,wv.n,6)
        i=pl.program_id(0)
        @pl.when(i==0)
        def _():
            c=wq.copies(wqr,w_s,sem.at[0])+wk.copies(wkr,w_s,sem.at[0],nq)+wv.copies(wvr,w_s,sem.at[0],nq+nk)
            fetch(c); acc[...]=jnp.zeros_like(acc); arrive(c)
        cos,sin=cos_ref[...],-sin_ref[...]
        for m in range(nq//HEAD):
            g_s[:,m*HEAD:(m+1)*HEAD]=turn(dq_ref[:,m*HEAD:(m+1)*HEAD].astype(f32),cos,sin).astype(bf16)
        for m in range(nk//HEAD):
            g_s[:,nq+m*HEAD:nq+(m+1)*HEAD]=turn(dk_ref[:,m*HEAD:(m+1)*HEAD].astype(f32),cos,sin).astype(bf16)
        g_s[:,nq+nk:]=dv_ref[...]
        acc[...]+=_dot(a_ref[...],g_s[...],0,0)
        by_a=_dot(g_s[...],w_s[...],1,1).astype(bf16).astype(f32)
        out_ref[...]=by_ref[...]+norm_back(by_a,h_ref[...].astype(f32)).astype(bf16)
        @pl.when(i==steps-1)
        def _(): dw_ref[...]=acc[...].astype(bf16)
    return pl.pallas_call(body,grid=(steps,),
        in_specs=[rows(bm,nq),rows(bm,nk),rows(bm,nk),rows(bm,d),rows(bm,d),rows(bm,d),rows(bm,HEAD),rows(bm,HEAD)]+[ANY]*(wq.n+wk.n+wv.n),
        out_specs=[rows(bm,d),whole((d,n))],out_shape=[jax.ShapeDtypeStruct((t,d),bf16),jax.ShapeDtypeStruct((d,n),bf16)],
        scratch_shapes=[pltpu.VMEM((d,n),bf16),pltpu.VMEM((bm,n),bf16),pltpu.VMEM((d,n),f32),pltpu.SemaphoreType.DMA((1,))],
        compiler_params=_params(),name="qkv_back",
        cost_estimate=_cost(4*t*d*n,2*(4*t*d+t*n+2*d*n)))(dq,dk,dv,a,h,by_h,cos,sin,*wq.pieces,*wk.pieces,*wv.pieces)

def solution(mesh):
    def whole(block, rows):
        size=block.shape[0]//2
        c=lax.rem(lax.axis_index("rep"),2)
        mine=lax.dynamic_slice_in_dim(block,c*size,size,0)
        got=lax.all_gather(mine,"dp",axis=0,tiled=True)
        other=lax.ppermute(got,"rep",[(r,r^1) for r in range(mesh.shape["rep"])])
        plan=[]
        for x in range(mesh.shape["dp"]):
            plan.append((0,x*size,size,lambda X,C,x=x: x*2*size+C*size))
            plan.append((1,x*size,size,lambda X,C,x=x: x*2*size+(1-C)*size))
        return Weight((block.shape[0]*mesh.shape["dp"],block.shape[1]),[got,other],plan)

    def step(x,dy,*weights):
        layers=weights[0].shape[0]
        by_name=dict(zip(NAMES,weights,strict=True))
        t=x.shape[1]
        half=HEAD//2
        angle=jnp.arange(t,dtype=f32)[:,None]*THETA**(-jnp.arange(half,dtype=f32)/half)
        cos,sin=jnp.cos(angle),jnp.sin(angle)
        cos,sin=jnp.concatenate([cos,cos],-1),jnp.concatenate([-sin,sin],-1)
        w=[{name: whole(by_name[name][n],None) for name in NAMES} for n in range(layers)]
        h=x[0]
        a,q,k,v=qkv(h,cos,sin,*(w[0][m] for m in("wq","wk","wv")))
        saved=[]
        for n in range(layers):
            o,lse=attend(q,k,v)
            h1,b=out_norm(o,h,w[n]["wo"])
            gate,up,act=mlp_in(b,w[n]["w_gate"],w[n]["w_up"])
            saved.append((h,a,q,k,v,o,lse,h1,b,gate,up,act))
            if n<layers-1: h,a,q,k,v=mlp_out_qkv(act,h1,w[n]["w_down"],cos,sin,*(w[n+1][m] for m in("wq","wk","wv")))
        by_h=dy[0]
        grads=[None]*layers
        scatter=lambda g: lax.psum_scatter(g,"dp",scatter_dimension=0,tiled=True)
        after=lambda value,done: lax.optimization_barrier((value,done))
        for n in reversed(range(layers)):
            h,a,q,k,v,o,lse,h1,b,gate,up,act=saved[n]; m=w[n]
            by_down=outer(act,by_h,640)
            by_h,by_down=after(by_h,by_down)
            s_down=scatter(by_down)
            by_gate,by_up,by_h1=mlp_back(by_h,gate,up,h1,m["w_gate"],m["w_up"],m["w_down"])
            g_gate=outer_k(b,by_gate)
            by_up,g_gate=after(by_up,g_gate)
            s_gate=scatter(g_gate)
            g_up=outer_k(b,by_up)
            by_h1,g_up=after(by_h1,g_up)
            s_up=scatter(g_up)
            by_o,g_o=out_back(by_h1,o,m["wo"])
            s_o=scatter(g_o)
            dq,dk,dv=attend_bwd(q,k,v,by_o,o,lse)
            by_h,g_qkv=qkv_back(dq,dk,dv,a,h,by_h1,cos,sin,m["wq"],m["wk"],m["wv"])
            s_qkv=scatter(g_qkv)
            nq,nk=m["wq"].shape[1],m["wk"].shape[1]
            grads[n]=(s_qkv[:,:nq],s_qkv[:,nq:nq+nk],s_qkv[:,nq+nk:],s_o,s_gate,s_up,s_down)
        return (by_h[None],*(jnp.stack([grads[n][i] for n in range(layers)]) for i in range(7)))

    states,cut=P(("rep","dp"),None,None),P(None,"dp",None)
    return jax.shard_map(step,mesh=mesh,in_specs=(states,states)+(cut,)*7,out_specs=(states,)+(P("rep","dp",None),)*7,check_vma=False)
```
